8 devices in a mesh: stage: 1 (over z), data: 8 (over y, x, core).
Axes of the slice: x: 2, y: 2, z: 1, core: 2. Of those that a mesh axis runs over, the one named last changes fastest.
Arguments:
- grad_attn: float32 [8, 2, 2048, 2048], P(('stage', 'data'))
- mom_attn: float32 [2, 2048, 2048], P('stage', 'data')
- master_attn: float32 [2, 2048, 2048], P('stage', 'data')
- grad_up: float32 [8, 4, 2048, 1408], P(('stage', 'data'))
- mom_up: float32 [4, 2048, 1408], P('stage', 'data')
- master_up: float32 [4, 2048, 1408], P('stage', 'data')
- grad_down: float32 [8, 4, 1408, 2048], P(('stage', 'data'))
- mom_down: float32 [4, 1408, 2048], P('stage', 'data')
- master_down: float32 [4, 1408, 2048], P('stage', 'data')
Outputs:
- output 1: float32 [2, 2048, 2048], P('stage', 'data')
- output 2: float32 [2, 2048, 2048], P('stage', 'data')
- output 3: bfloat16 [2, 2048, 2048], P('stage', 'data')
- output 4: float32 [4, 2048, 1408], P('stage', 'data')
- output 5: float32 [4, 2048, 1408], P('stage', 'data')
- output 6: bfloat16 [4, 2048, 1408], P('stage', 'data')
- output 7: float32 [4, 1408, 2048], P('stage', 'data')
- output 8: float32 [4, 1408, 2048], P('stage', 'data')
- output 9: bfloat16 [4, 1408, 2048], P('stage', 'data')
All inputs are finite; a program needn't handle non-finite values.
Results may differ from the reference program's by a relative error of at most 0.00648393.
Values are sent between devices in bfloat16 or wider.
A program may use at most 1 GiB of HBM per device.

```python
import math
import jax
import jax.numpy as jnp
from jax import lax

HIDDEN = 2048
FFN_WIDTH = 1408
ATTN_COUNT = 2
EXPERT_COUNT = 4
GROUP_SIZE = 8
NS_STEPS = 5

MOMENTUM = 0.95
LEARN_RATE = 0.25
WEIGHT_DECAY = 0.2
EPSILON = 1e-7
COEF_A = 3.4445
COEF_B = -4.7750
COEF_C = 2.0315
STACK_SHAPES = ((ATTN_COUNT, HIDDEN, HIDDEN), (EXPERT_COUNT, HIDDEN, FFN_WIDTH), (EXPERT_COUNT, FFN_WIDTH, HIDDEN))
STACK_NAMES = ('attn', 'up', 'down')


def draw_grads(key, count, n_rows, n_cols):
    noise = jax.random.normal(key, (GROUP_SIZE, count, n_rows, n_cols), jnp.float32)
    row_owner = jnp.arange(n_rows) // (n_rows // GROUP_SIZE)
    scale = jnp.where(row_owner[None, :] == jnp.arange(GROUP_SIZE)[:, None], 0.8 * GROUP_SIZE, 0.5)
    return noise * scale[:, None, :, None]


def setup_inputs(seed: int = 0, part: int = 0) -> dict:
    base_key = jax.random.fold_in(jax.random.key(seed), part)
    keys = jax.random.split(base_key, 9)
    inputs = {}
    for stack_idx in range(3):
        count, n_rows, n_cols = STACK_SHAPES[stack_idx]
        label = STACK_NAMES[stack_idx]
        inputs['grad_' + label] = draw_grads(keys[3 * stack_idx], count, n_rows, n_cols)
        inputs['mom_' + label] = jax.random.normal(keys[3 * stack_idx + 1], (count, n_rows, n_cols), jnp.float32)
        inputs['master_' + label] = 0.5 * jax.random.normal(keys[3 * stack_idx + 2], (count, n_rows, n_cols), jnp.float32)
    return inputs


def orthogonalize(mom_new):
    n_rows, n_cols = mom_new.shape
    norm = jnp.sqrt(jnp.sum(mom_new * mom_new))
    x_mat = (mom_new / (norm + EPSILON)).astype(jnp.bfloat16)
    if n_rows > n_cols:
        x_mat = x_mat.T
    for _ in range(NS_STEPS):
        gram_mat = jnp.dot(x_mat, x_mat.T, preferred_element_type=jnp.float32).astype(jnp.bfloat16)
        gram_sq = jnp.dot(gram_mat, gram_mat, preferred_element_type=jnp.float32).astype(jnp.bfloat16)
        poly_mat = (COEF_B * gram_mat.astype(jnp.float32) + COEF_C * gram_sq.astype(jnp.float32)).astype(jnp.bfloat16)
        update = jnp.dot(poly_mat, x_mat, preferred_element_type=jnp.float32).astype(jnp.bfloat16)
        x_mat = (COEF_A * x_mat.astype(jnp.float32) + update.astype(jnp.float32)).astype(jnp.bfloat16)
    if n_rows > n_cols:
        x_mat = x_mat.T
    return x_mat


def stack_step(grad_all, mom_old, master_old):
    n_rows, n_cols = mom_old.shape[1], mom_old.shape[2]
    grad_mean = jnp.sum(grad_all, axis=0) / GROUP_SIZE
    mom_new = MOMENTUM * mom_old + grad_mean
    ortho_mat = lax.map(orthogonalize, mom_new)
    scale = 0.2 * math.sqrt(max(n_rows, n_cols))
    master_new = master_old - LEARN_RATE * (scale * ortho_mat.astype(jnp.float32) + WEIGHT_DECAY * master_old)
    return mom_new, master_new, master_new.astype(jnp.bfloat16)


def reference(grad_attn, mom_attn, master_attn, grad_up, mom_up, master_up, grad_down, mom_down, master_down):
    attn_out = stack_step(grad_attn, mom_attn, master_attn)
    up_out = stack_step(grad_up, mom_up, master_up)
    down_out = stack_step(grad_down, mom_down, master_down)
    return (attn_out[0], attn_out[1], attn_out[2], up_out[0], up_out[1], up_out[2], down_out[0], down_out[1], down_out[2])
```

```python
import math
import functools
import jax
import jax.numpy as jnp
from jax import lax
from jax.experimental import pallas as pl
from jax.experimental.pallas import tpu as pltpu
from jax.experimental.layout import Layout, with_layout_constraint
from jax.sharding import PartitionSpec as P

MOMENTUM = 0.95
LEARN_RATE = 0.25
WEIGHT_DECAY = 0.2
EPSILON = 1e-7
COEF_A = 3.4445
COEF_B = -4.7750
COEF_C = 2.0315
NS_STEPS = 5
GROUP = 8
FIRST_JOBS = ((0, 0, 0, 0), (0, 1, 3, 0), (1, 0, 1, 0), (1, 2, 2, 0), (1, 1, 1, 1), (1, 3, 2, 1))
LAST_JOBS = ((0, 0, 0, 0), (0, 1, 1, 0), (0, 2, 2, 0), (0, 3, 3, 0))


def greet_all(me):
    barrier = pltpu.get_barrier_semaphore()
    for step in range(1, GROUP):
        pl.semaphore_signal(barrier, inc=1, device_id={'data': lax.rem(me + step, GROUP)}, device_id_type=pl.DeviceIdType.MESH)
    pl.semaphore_wait(barrier, GROUP - 1)


def share_kernel(part_ref, all_ref, send_sem, recv_sem):
    me = lax.axis_index('data')
    greet_all(me)
    copies = []
    for step in range(1, GROUP):
        copies.append(pltpu.make_async_remote_copy(
            src_ref=part_ref, dst_ref=all_ref.at[step], send_sem=send_sem.at[step], recv_sem=recv_sem.at[step],
            device_id={'data': lax.rem(me + step, GROUP)}, device_id_type=pl.DeviceIdType.MESH))
    for copy in copies:
        copy.start()
    all_ref[0] = part_ref[...]
    for copy in copies:
        copy.wait()


def sum_over_data(partial, collective_id):
    count = partial.shape[0]
    tile = jnp.broadcast_to(jnp.pad(partial, (0, 8 - count))[:, None], (8, 128))
    shared = pl.pallas_call(
        share_kernel,
        out_shape=jax.ShapeDtypeStruct((GROUP, 8, 128), jnp.float32),
        in_specs=[pl.BlockSpec(memory_space=pltpu.VMEM)],
        out_specs=pl.BlockSpec(memory_space=pltpu.VMEM),
        scratch_shapes=[pltpu.SemaphoreType.DMA((GROUP,)), pltpu.SemaphoreType.DMA((GROUP,))],
        compiler_params=pltpu.CompilerParams(collective_id=collective_id, has_side_effects=True),
        cost_estimate=pl.CostEstimate(flops=20_000_000, bytes_accessed=65536, transcendentals=0),
        name=f'share{collective_id}',
    )(tile)
    me = lax.axis_index('data')
    ordered = jnp.take(shared[:, :, 0], lax.rem(me - jnp.arange(GROUP) + GROUP, GROUP), axis=0)
    return jnp.sum(ordered, axis=0)[:count]


def block_of(ref, device, size, axis):
    start = pl.multiple_of(device * size, size)
    return ref.at[pl.ds(start, size), :] if axis == 0 else ref.at[:, pl.ds(start, size)]


def ortho_kernel(jobs, *refs):
    n_stacks = 1 + max(job[0] for job in jobs)
    ins, outs = refs[:n_stacks], refs[n_stacks:2 * n_stacks]
    (x_ref, a_ref, b_ref, send_sem, recv_sem, pass_sem, passed_sem, back_sem, got_sem, own_sem, tile_send, tile_recv) = refs[2 * n_stacks:]
    me = lax.axis_index('data')
    chip, core = me // 2, me % 2
    partner = me + 1 - 2 * core
    greet_all(me)
    n_long = x_ref.shape[3]
    chips = GROUP // 2
    last = NS_STEPS % 2

    def remote(src, dst, send, recv, target):
        return pltpu.make_async_remote_copy(src_ref=src, dst_ref=dst, send_sem=send, recv_sem=recv,
                                            device_id={'data': target}, device_id_type=pl.DeviceIdType.MESH)

    def block(job, slot, device):
        _, _, _, turn, axis, n_short = jobs[job]
        size = (n_short if axis == 0 else n_long) // GROUP
        return block_of(x_ref.at[turn, slot, pl.ds(0, n_short)], device, size, axis)

    def rows_in(job):
        return ins[jobs[job][0]].at[jobs[job][1]]

    def rows_out(job):
        return outs[jobs[job][0]].at[jobs[job][1]]

    def collect(job, source):
        return remote(rows_in(job), block(job, 0, 2 * source + core), send_sem.at[job], recv_sem.at[job, source], 2 * jobs[job][2] + core)

    def collect_own(job):
        return pltpu.make_async_copy(rows_in(job), block(job, 0, me), own_sem.at[job])

    def pass_on(job, source, side):
        there = block(job, 0, 2 * source + side)
        return remote(there, there, pass_sem.at[job, source], passed_sem.at[job, source], partner)

    def hand_out(job, target):
        return remote(block(job, last, 2 * target + core), rows_out(job), back_sem.at[job, target], got_sem.at[job], 2 * target + core)

    def hand_out_own(job):
        return pltpu.make_async_copy(block(job, last, me), rows_out(job), own_sem.at[job])

    for job, (_, _, owner, turn, _, n_short) in enumerate(jobs):
        @pl.when(chip != owner)
        def _():
            collect(job, chip).start()

        @pl.when(chip == owner)
        def _():
            collect_own(job).start()
            n_pad = padded(n_short)
            if n_pad > n_short:
                for slot in range(2):
                    x_ref[turn, slot, n_short:n_pad, :] = jnp.zeros((n_pad - n_short, n_long), jnp.bfloat16)

    for turn in range(x_ref.shape[0]):
        mine = [job for job in range(len(jobs)) if jobs[job][3] == turn]
        for job in mine:
            owner = jobs[job][2]

            @pl.when(chip == owner)
            def _():
                collect_own(job).wait()
                pass_on(job, owner, core).start()
                for source in range(chips):
                    if source != owner:
                        collect(job, source).wait_recv()
                        pass_on(job, source, core).start()
                for source in range(chips):
                    pass_on(job, source, core).wait_send()
                    pass_on(job, source, 1 - core).wait_recv()
        for n_short in sorted({jobs[job][5] for job in mine}):
            @pl.when(functools.reduce(jnp.logical_or, [chip == jobs[job][2] for job in mine if jobs[job][5] == n_short]))
            def _():
                n_pad = padded(n_short)
                square = pl.ds(0, n_pad)
                step = functools.partial(ns_step, n_short, core, partner, remote, x_ref.at[turn, :, pl.ds(0, n_pad)],
                                         a_ref.at[square, square], b_ref.at[square, square], tile_send, tile_recv)
                lax.fori_loop(0, NS_STEPS, step, 0)
        for job in mine:
            owner = jobs[job][2]

            @pl.when(chip == owner)
            def _():
                for target in range(chips):
                    (hand_out_own(job) if target == owner else hand_out(job, target)).start()

    for job, (_, _, owner, _, _, _) in enumerate(jobs):
        @pl.when(chip == owner)
        def _():
            hand_out_own(job).wait()
            for target in range(chips):
                if target != owner:
                    hand_out(job, target).wait_send()

        @pl.when(chip != owner)
        def _():
            collect(job, chip).wait_send()
            hand_out(job, chip).wait_recv()


def padded(n_short):
    return -(-n_short // TILE) * TILE


TILE = 512


def ns_step(n_short, core, partner, remote, x_ref, a_ref, b_ref, tile_send, tile_recv, step, carry):
    n_pad, n_long = x_ref.shape[1:]
    x_now, x_next = x_ref.at[step % 2], x_ref.at[(step + 1) % 2]
    tiles = n_pad // TILE

    def span(i, length=TILE):
        return pl.ds(pl.multiple_of(i * length, length), length)

    def send(stage, ref):
        remote(ref, ref, tile_send.at[stage], tile_recv.at[stage], partner).start()

    def await_tiles(stage, sent, received):
        def view(count):
            return x_ref.at[0, pl.ds(0, count * TILE * TILE // n_long), :]
        for side in range(2):
            @pl.when(core == side)
            def _():
                remote(view(sent[side]), view(sent[side]), tile_send.at[stage], tile_recv.at[stage], partner).wait_send()
                remote(view(received[side]), view(received[side]), tile_send.at[stage], tile_recv.at[stage], partner).wait_recv()

    def owner_of(i, j):
        return (i // 2 + j) % 2

    def upper(stage, ref, body):
        def visit(t, c):
            i, j = t // tiles, t % tiles

            @pl.when(jnp.logical_and(i <= j, owner_of(i, j) == core))
            def _():
                tile = body(i, j)
                ref[span(i), span(j)] = tile
                send(stage, ref.at[span(i), span(j)])

                @pl.when(i != j)
                def _():
                    ref[span(j), span(i)] = tile.T
                    send(stage, ref.at[span(j), span(i)])
            return c
        lax.fori_loop(0, tiles * tiles, visit, 0)
        count = [sum(1 + (i != j) for i in range(tiles) for j in range(i, tiles) if owner_of(i, j) == side) for side in range(2)]
        await_tiles(stage, count, count[::-1])

    def gram(i, j):
        tile = lax.dot_general(x_now[span(i), :], x_now[span(j), :], (((1,), (1,)), ((), ())), preferred_element_type=jnp.float32)
        return tile.astype(jnp.bfloat16)

    def poly(i, j):
        square = jnp.dot(a_ref[span(i), :n_short], a_ref[:n_short, span(j)], preferred_element_type=jnp.float32)
        tile = COEF_B * a_ref[span(i), span(j)].astype(jnp.float32) + COEF_C * square.astype(jnp.bfloat16).astype(jnp.float32)
        return tile.astype(jnp.bfloat16)

    upper(0, a_ref, gram)
    upper(1, b_ref, poly)
    height = n_short // 2
    wide = n_long // TILE // 2

    def apply(t, c):
        rows, cols = span(t // wide, height), span(core * wide + t % wide)
        update = jnp.dot(b_ref[rows, :n_short], x_now[:n_short, cols], preferred_element_type=jnp.float32).astype(jnp.bfloat16)
        x_next[rows, cols] = (COEF_A * x_now[rows, cols].astype(jnp.float32) + update.astype(jnp.float32)).astype(jnp.bfloat16)
        send(2, x_next.at[rows, cols])
        return c

    lax.fori_loop(0, 2 * wide, apply, 0)
    half = x_ref.at[0, pl.ds(0, n_short // 2), :]
    remote(half, half, tile_send.at[2], tile_recv.at[2], partner).wait()
    return carry


def orthogonalize(jobs, stacks, collective_id):
    shorts = [rows.shape[1] * (GROUP if axis == 0 else 1) for rows, axis in stacks]
    n_long = stacks[0][0].shape[2] * (GROUP if stacks[0][1] == 1 else 1)
    full = [(stack, k, chip, turn, stacks[stack][1], shorts[stack]) for stack, k, chip, turn in jobs]
    n_pad = padded(max(shorts))
    turns = 1 + max(job[3] for job in jobs)
    n_jobs, chips = len(jobs), GROUP // 2
    dma = pltpu.SemaphoreType.DMA
    return pl.pallas_call(
        functools.partial(ortho_kernel, full),
        out_shape=[jax.ShapeDtypeStruct(rows.shape, rows.dtype) for rows, _ in stacks],
        in_specs=[pl.BlockSpec(memory_space=pl.ANY)] * len(stacks),
        out_specs=[pl.BlockSpec(memory_space=pl.ANY)] * len(stacks),
        scratch_shapes=[pltpu.VMEM((turns, 2, n_pad, n_long), jnp.bfloat16), pltpu.VMEM((n_pad, n_pad), jnp.bfloat16),
                        pltpu.VMEM((n_pad, n_pad), jnp.bfloat16),
                        dma((n_jobs,)), dma((n_jobs, chips)), dma((n_jobs, chips)), dma((n_jobs, chips)), dma((n_jobs, chips)),
                        dma((n_jobs,)), dma((n_jobs,)), dma((3,)), dma((3,))],
        compiler_params=pltpu.CompilerParams(collective_id=collective_id, has_side_effects=True, vmem_limit_bytes=58 << 20),
        cost_estimate=pl.CostEstimate(flops=2_000_000_000, bytes_accessed=16 << 20, transcendentals=0),
        name=f'ortho{collective_id}',
    )(*[rows for rows, _ in stacks])


SLOTS = 5


def reduce_kernel(n_chunks, per_matrix, grad_ref, out_ref, own_ref, pair_ref, first_ref, second_ref, sum_ref,
                  load_sem, pair_send, pair_recv, first_send, first_recv, second_send, second_recv, out_sem):
    me = lax.axis_index('data')
    y, x, core = me // 4, (me // 2) % 2, me % 2
    greet_all(me)
    chunk = own_ref.shape[3]
    half = chunk // 2
    parts = (pl.ds(0, half), pl.ds(half, half))
    over_core, over_x, over_y = me + 1 - 2 * core, me + 2 - 4 * x, me + 4 - 8 * y

    def remote(src, dst, send, recv, target):
        return pltpu.make_async_remote_copy(src_ref=src, dst_ref=dst, send_sem=send, recv_sem=recv,
                                            device_id={'data': target}, device_id_type=pl.DeviceIdType.MESH)

    def rows_of(c):
        return pl.ds(pl.multiple_of((c % per_matrix) * chunk, chunk), chunk)

    def load(c):
        return pltpu.make_async_copy(grad_ref.at[c // per_matrix, :, :, core, rows_of(c)], own_ref.at[c % SLOTS], load_sem.at[c % SLOTS])

    def pair(c):
        return remote(grad_ref.at[c // per_matrix, :, :, 1 - core, rows_of(c)], pair_ref.at[c % SLOTS],
                      pair_send.at[c % SLOTS], pair_recv.at[c % SLOTS], over_core)

    def first(c):
        slot = c % SLOTS
        return (remote(own_ref.at[slot, :, 1 - x, parts[0]], first_ref.at[slot, 0], first_send.at[slot, 0], first_recv.at[slot, 0], over_x),
                remote(own_ref.at[slot, 1 - y, :, parts[1]], first_ref.at[slot, 1], first_send.at[slot, 1], first_recv.at[slot, 1], over_y))

    def second(c):
        slot = c % SLOTS
        return (remote(own_ref.at[slot, 1 - y, x, parts[0]], second_ref.at[slot, 0], second_send.at[slot, 0], second_recv.at[slot, 0], over_y),
                remote(own_ref.at[slot, y, 1 - x, parts[1]], second_ref.at[slot, 1], second_send.at[slot, 1], second_recv.at[slot, 1], over_x))

    def store(c):
        return pltpu.make_async_copy(sum_ref.at[c % SLOTS], out_ref.at[c // per_matrix, rows_of(c)], out_sem.at[c % SLOTS])

    def during(c, body):
        pl.when(jnp.logical_and(c >= 0, c < n_chunks))(lambda: body(c))

    def finish(c):
        slot = c % SLOTS
        for copy in second(c):
            copy.wait()
        pl.when(c >= SLOTS)(lambda: store(c - SLOTS).wait())
        for side in range(2):
            sum_ref[slot, parts[side]] = own_ref[slot, y, x, parts[side]] + second_ref[slot, side]
        store(c).start()

    def middle(c):
        slot = c % SLOTS
        for copy in first(c):
            copy.wait()
        for other in range(2):
            own_ref[slot, other, x, parts[0]] += first_ref[slot, 0, other]
            own_ref[slot, y, other, parts[1]] += first_ref[slot, 1, other]
        for copy in second(c):
            copy.start()

    def begin(c):
        slot = c % SLOTS
        load(c).wait()
        pair(c).wait()
        own_ref[slot] += pair_ref[slot]
        for copy in first(c):
            copy.start()

    def fetch(c):
        load(c).start()
        pair(c).start()

    def visit(t, carry):
        during(t - 5, finish)
        during(t - 3, middle)
        during(t - 1, begin)
        during(t, fetch)
        return carry

    lax.fori_loop(0, n_chunks + 5, visit, 0)
    for c in range(max(0, n_chunks - SLOTS), n_chunks):
        store(c).wait()


def reduce_rows_kernel(grad, chunk, collective_id):
    count, n_rows, n_cols = grad.shape
    rows = n_rows // GROUP
    per_matrix = rows // chunk
    dma, vmem = pltpu.SemaphoreType.DMA, lambda *shape: pltpu.VMEM(shape, jnp.float32)
    return pl.pallas_call(
        functools.partial(reduce_kernel, count * per_matrix, per_matrix),
        out_shape=jax.ShapeDtypeStruct((count, rows, n_cols), jnp.float32),
        in_specs=[pl.BlockSpec(memory_space=pl.ANY)],
        out_specs=pl.BlockSpec(memory_space=pl.ANY),
        scratch_shapes=[vmem(SLOTS, 2, 2, chunk, n_cols), vmem(SLOTS, 2, 2, chunk, n_cols), vmem(SLOTS, 2, 2, chunk // 2, n_cols),
                        vmem(SLOTS, 2, chunk // 2, n_cols), vmem(SLOTS, chunk, n_cols),
                        dma((SLOTS,)), dma((SLOTS,)), dma((SLOTS,)), dma((SLOTS, 2)), dma((SLOTS, 2)), dma((SLOTS, 2)), dma((SLOTS, 2)),
                        dma((SLOTS,))],
        compiler_params=pltpu.CompilerParams(collective_id=collective_id, has_side_effects=True, vmem_limit_bytes=40 << 20),
        cost_estimate=pl.CostEstimate(flops=1_000_000_000, bytes_accessed=64 << 20, transcendentals=0),
        name=f'reduce{collective_id}',
    )(grad.reshape(count, 2, 2, 2, rows, n_cols))


def momentum(grad_rows, mom_old):
    mom_new = MOMENTUM * mom_old + grad_rows / GROUP
    return mom_new, jnp.sum(mom_new * mom_new, axis=(1, 2))


def to_send(mom_new, norm_sq, transposed):
    x_rows = (mom_new / (jnp.sqrt(norm_sq)[:, None, None] + EPSILON)).astype(jnp.bfloat16)
    return jnp.swapaxes(x_rows, 1, 2) if transposed else x_rows


def new_weights(ortho_rows, master_old, n_rows, n_cols):
    scale = 0.2 * math.sqrt(max(n_rows, n_cols))
    master_new = master_old - LEARN_RATE * (scale * ortho_rows.astype(jnp.float32) + WEIGHT_DECAY * master_old)
    return master_new, master_new.astype(jnp.bfloat16)


def solution(mesh):
    grad_spec = P(('stage', 'data'), None, None, None)
    row_spec = P('stage', 'data', None)

    def step_local(g_attn, m_attn, w_attn, g_up, m_up, w_up, g_down, m_down, w_down):
        def reduce_rows(grad):
            return lax.psum_scatter(grad[0], 'data', scatter_dimension=1, tiled=True)

        r_attn = reduce_rows(g_attn)
        r_down = reduce_rows(g_down)
        r_up = reduce_rows_kernel(g_up[0], 32, 7)
        r_attn, r_up = lax.optimization_barrier((r_attn, r_up))

        mn_attn, part_attn = momentum(r_attn, m_attn)
        mn_up, part_up = momentum(r_up, m_up)
        mn_up = with_layout_constraint(mn_up, Layout((0, 1, 2)))
        parts = sum_over_data(jnp.concatenate([part_attn, part_up]), 0)
        x_attn = to_send(mn_attn, parts[:2], False)
        x_up = to_send(mn_up, parts[2:], True)
        or_attn, or_up = orthogonalize(FIRST_JOBS, [(x_attn, 0), (x_up, 1)], 1)
        wn_attn, wb_attn = new_weights(or_attn, w_attn, 2048, 2048)
        wn_up, wb_up = new_weights(jnp.swapaxes(or_up, 1, 2), w_up, 2048, 1408)

        r_down, wn_attn, wb_attn, wn_up, wb_up = lax.optimization_barrier((r_down, wn_attn, wb_attn, wn_up, wb_up))
        mn_down, part_down = momentum(r_down, m_down)
        x_down = to_send(mn_down, sum_over_data(part_down, 4), False)
        or_down, = orthogonalize(LAST_JOBS, [(x_down, 0)], 5)
        wn_down, wb_down = new_weights(or_down, w_down, 1408, 2048)
        return (mn_attn, wn_attn, wb_attn, mn_up, wn_up, wb_up, mn_down, wn_down, wb_down)

    in_specs = (grad_spec, row_spec, row_spec) * 3
    out_specs = (row_spec,) * 9
    return jax.shard_map(step_local, mesh=mesh, in_specs=in_specs, out_specs=out_specs, check_vma=False)
```

```python
import math
import functools
import jax
import jax.numpy as jnp
from jax import lax
from jax.experimental import pallas as pl
from jax.experimental.pallas import tpu as pltpu
from jax.sharding import PartitionSpec as P

MOMENTUM = 0.95
LEARN_RATE = 0.25
WEIGHT_DECAY = 0.2
EPSILON = 1e-7
COEF_A = 3.4445
COEF_B = -4.7750
COEF_C = 2.0315
NS_STEPS = 5
GROUP = 8
FIRST_JOBS = ((0, 0, 0, 0), (0, 1, 3, 0), (1, 0, 1, 0), (1, 2, 2, 0), (1, 1, 1, 1), (1, 3, 2, 1))
LAST_JOBS = ((0, 0, 0, 0), (0, 1, 1, 0), (0, 2, 2, 0), (0, 3, 3, 0))


def greet_all(me):
    barrier = pltpu.get_barrier_semaphore()
    for step in range(1, GROUP):
        pl.semaphore_signal(barrier, inc=1, device_id={'data': lax.rem(me + step, GROUP)}, device_id_type=pl.DeviceIdType.MESH)
    pl.semaphore_wait(barrier, GROUP - 1)


def share_kernel(part_ref, all_ref, send_sem, recv_sem):
    me = lax.axis_index('data')
    greet_all(me)
    copies = []
    for step in range(1, GROUP):
        copies.append(pltpu.make_async_remote_copy(
            src_ref=part_ref, dst_ref=all_ref.at[step], send_sem=send_sem.at[step], recv_sem=recv_sem.at[step],
            device_id={'data': lax.rem(me + step, GROUP)}, device_id_type=pl.DeviceIdType.MESH))
    for copy in copies:
        copy.start()
    all_ref[0] = part_ref[...]
    for copy in copies:
        copy.wait()


def sum_over_data(partial, collective_id):
    count = partial.shape[0]
    tile = jnp.broadcast_to(jnp.pad(partial, (0, 8 - count))[:, None], (8, 128))
    shared = pl.pallas_call(
        share_kernel,
        out_shape=jax.ShapeDtypeStruct((GROUP, 8, 128), jnp.float32),
        in_specs=[pl.BlockSpec(memory_space=pltpu.VMEM)],
        out_specs=pl.BlockSpec(memory_space=pltpu.VMEM),
        scratch_shapes=[pltpu.SemaphoreType.DMA((GROUP,)), pltpu.SemaphoreType.DMA((GROUP,))],
        compiler_params=pltpu.CompilerParams(collective_id=collective_id, has_side_effects=True),
        cost_estimate=pl.CostEstimate(flops=20_000_000, bytes_accessed=65536, transcendentals=0),
        name=f'share{collective_id}',
    )(tile)
    me = lax.axis_index('data')
    ordered = jnp.take(shared[:, :, 0], lax.rem(me - jnp.arange(GROUP) + GROUP, GROUP), axis=0)
    return jnp.sum(ordered, axis=0)[:count]


def block_of(ref, device, size, axis):
    start = pl.multiple_of(device * size, size)
    return ref.at[pl.ds(start, size), :] if axis == 0 else ref.at[:, pl.ds(start, size)]


def ortho_kernel(jobs, late, keep, *refs):
    n_stacks = 1 + max(job[0] for job in jobs)
    n_late = 1 + max([job[0] for job in late], default=-1)
    n_in = n_stacks + (n_late > 0)
    n_out = 1 if keep else n_stacks
    ins, kept_in = refs[:n_stacks], refs[n_in - 1]
    outs, late_outs = refs[n_in:n_in + n_out], refs[n_in + n_out:n_in + n_out + n_late]
    scratch = refs[n_in + n_out + n_late:]
    (x_ref, a_ref, b_ref, far_ref, send_sem, recv_sem, pass_sem, passed_sem, back_sem, got_sem, own_sem,
     tile_send, tile_recv) = scratch[:13]
    me = lax.axis_index('data')
    chip, core = me // 2, me % 2
    partner = me + 1 - 2 * core
    greet_all(me)
    n_long = x_ref.shape[1]
    chips = GROUP // 2
    turn_rows = rows_of_turn(jobs, 0)
    last = NS_STEPS % 2

    def remote(src, dst, send, recv, target):
        return pltpu.make_async_remote_copy(src_ref=src, dst_ref=dst, send_sem=send, recv_sem=recv,
                                            device_id={'data': target}, device_id_type=pl.DeviceIdType.MESH)

    def block(job, slot, device):
        _, _, _, turn, axis, n_short = jobs[job]
        size = (n_short if axis == 0 else n_long) // GROUP
        return block_of(x_ref.at[pl.ds(turn * turn_rows + slot * padded(n_short), n_short)], device, size, axis)

    def rows_in(job):
        return ins[jobs[job][0]].at[jobs[job][1]]

    def rows_out(job):
        return outs[jobs[job][0]].at[jobs[job][1]]

    def collect(job, source):
        return remote(rows_in(job), block(job, 0, 2 * source + core), send_sem.at[job], recv_sem.at[job, source], 2 * jobs[job][2] + core)

    def collect_own(job):
        return pltpu.make_async_copy(rows_in(job), block(job, 0, me), own_sem.at[job])

    def pass_on(job, source, side):
        there = block(job, 0, 2 * source + side)
        return remote(there, there, pass_sem.at[job, source], passed_sem.at[job, source], partner)

    def hand_out(job, target):
        return remote(block(job, last, 2 * target + core), rows_out(job), back_sem.at[job, target], got_sem.at[job], 2 * target + core)

    def hand_out_own(job):
        return pltpu.make_async_copy(block(job, last, me), rows_out(job), own_sem.at[job])

    def store(job):
        _, _, _, turn, _, n_short = jobs[job]
        there = x_ref.at[pl.ds(turn * turn_rows + last * padded(n_short), n_short)]
        return pltpu.make_async_copy(there, outs[0].at[pl.ds(turn * n_short, n_short)], own_sem.at[job])

    def late_block(index, device):
        _, _, _, turn, axis, n_short = late[index]
        size = (n_short if axis == 0 else n_long) // GROUP
        return block_of(kept_in.at[pl.ds(turn * n_short, n_short)], device, size, axis)

    def late_out(index):
        return late_outs[late[index][0]].at[late[index][1]]

    def late_hand_out(index, target):
        return remote(late_block(index, 2 * target + core), late_out(index), scratch[13].at[index, target], scratch[14].at[index], 2 * target + core)

    def late_own(index, outward):
        room = scratch[16 + late[index][0]].at[late[index][3]]
        if outward:
            return pltpu.make_async_copy(room, late_out(index), scratch[15].at[index, 1])
        return pltpu.make_async_copy(late_block(index, me), room, scratch[15].at[index, 0])

    def each_late(owning, other=None):
        for index, job in enumerate(late):
            pl.when(chip == job[2])(functools.partial(owning, index))
            if other is not None:
                pl.when(chip != job[2])(functools.partial(other, index))

    def late_begin(index):
        late_own(index, False).start()
        for target in range(chips):
            if target != late[index][2]:
                late_hand_out(index, target).start()

    def late_middle(index):
        late_own(index, False).wait()
        late_own(index, True).start()

    def late_end(index):
        late_own(index, True).wait()
        for target in range(chips):
            if target != late[index][2]:
                late_hand_out(index, target).wait_send()

    for job, (_, _, owner, turn, _, n_short) in enumerate(jobs):
        @pl.when(chip != owner)
        def _():
            collect(job, chip).start()

        @pl.when(chip == owner)
        def _():
            collect_own(job).start()
            n_pad = padded(n_short)
            if n_pad > n_short:
                for slot in range(2):
                    start = turn * turn_rows + slot * n_pad
                    x_ref[start + n_short:start + n_pad, :] = jnp.zeros((n_pad - n_short, n_long), jnp.bfloat16)

    def receive(job):
        collect_own(job).wait()
        pass_on(job, jobs[job][2], core).start()
        for source in range(chips):
            if source != jobs[job][2]:
                collect(job, source).wait_recv()
                pass_on(job, source, core).start()
        for source in range(chips):
            pass_on(job, source, core).wait_send()
            pass_on(job, source, 1 - core).wait_recv()

    def give_back(job):
        if keep:
            store(job).start()
            return
        for target in range(chips):
            (hand_out_own(job) if target == jobs[job][2] else hand_out(job, target)).start()

    for n_short in sorted({job[5] for job in jobs}):
        mine = [job for job in range(len(jobs)) if jobs[job][5] == n_short]

        def work(turn, carry):
            def each(body):
                for job in mine:
                    pl.when(jnp.logical_and(chip == jobs[job][2], turn == jobs[job][3]))(functools.partial(body, job))

            each(receive)
            each_late(late_begin)
            newton_schulz(padded(n_short) // 2, core, partner, remote, x_ref, turn * turn_rows, a_ref, b_ref, far_ref, tile_send, tile_recv)
            each(give_back)
            each_late(late_middle)
            return carry

        @pl.when(functools.reduce(jnp.logical_or, [chip == jobs[job][2] for job in mine]))
        def _():
            lax.fori_loop(0, 1 + max(jobs[job][3] for job in mine), work, 0)

    for job, (_, _, owner, _, _, _) in enumerate(jobs):
        @pl.when(chip == owner)
        def _():
            if keep:
                store(job).wait()
                return
            hand_out_own(job).wait()
            for target in range(chips):
                if target != owner:
                    hand_out(job, target).wait_send()

        @pl.when(chip != owner)
        def _():
            collect(job, chip).wait_send()
            if not keep:
                hand_out(job, chip).wait_recv()
    each_late(late_end, lambda index: late_hand_out(index, chip).wait_recv())


def padded(n_short):
    return -(-n_short // TILE) * TILE


def rows_of_turn(jobs, turn):
    return 2 * padded(max([job[5] for job in jobs if job[3] == turn], default=0))


TILE = 512


def newton_schulz(half, core, partner, remote, x_ref, base, a_ref, b_ref, far_ref, tile_send, tile_recv):
    n_long = x_ref.shape[1]
    near, far = (pl.ds(pl.multiple_of(side * half, half), half) for side in (core, 1 - core))
    mine = pl.ds(0, half)

    def rows(slot, side):
        return pl.ds(pl.multiple_of(base + (2 * slot + side) * half, 256), half)

    def a_copy(parity):
        return remote(a_ref.at[mine, near], far_ref.at[parity, mine, mine], tile_send.at[parity], tile_recv.at[parity], partner)

    def x_copy(slot, columns):
        there = x_ref.at[rows(slot, core), columns]
        return remote(there, there, tile_send.at[2 + slot], tile_recv.at[2 + slot], partner)

    def dot(left, right):
        return jnp.dot(left, right, preferred_element_type=jnp.float32)

    def dot_t(left, right):
        return lax.dot_general(left, right, (((1,), (1,)), ((), ())), preferred_element_type=jnp.float32)

    def piece(index):
        return pl.ds(pl.multiple_of(index * (half // 2), half // 2), half // 2)

    def poly(columns, square):
        def visit(index, c):
            band = piece(index)
            tile = COEF_B * a_ref[band, columns].astype(jnp.float32)
            tile += COEF_C * square(band).astype(jnp.bfloat16).astype(jnp.float32)
            b_ref[band, columns] = tile.astype(jnp.bfloat16)
            return c
        lax.fori_loop(0, 2, visit, 0)

    def step(count, carry):
        now, later = count % 2, (count + 1) % 2

        def gram(turn, c):
            side = core + (turn // 2) * (1 - 2 * core)
            band, columns = piece(turn % 2), pl.ds(pl.multiple_of(side * half, half), half)
            left = x_ref[pl.ds(pl.multiple_of(base + (2 * now + core) * half + (turn % 2) * (half // 2), 128), half // 2), :]
            a_ref[band, columns] = dot_t(left, x_ref[rows(now, side), :]).astype(jnp.bfloat16)
            pl.when(turn == 1)(lambda: a_copy(now).start())
            pl.when(jnp.logical_and(turn == 1, count > 0))(lambda: x_copy(now, pl.ds(0, n_long)).wait())
            return c

        lax.fori_loop(0, 4, gram, 0)
        poly(near, lambda band: dot(a_ref[band, near], a_ref[mine, near]) + dot_t(a_ref[band, far], a_ref[mine, far]))
        a_copy(now).wait()
        poly(far, lambda band: dot(a_ref[band, near], a_ref[mine, far]) + dot(a_ref[band, far], far_ref[now, mine, mine]))

        def apply(t, c):
            columns = pl.ds(pl.multiple_of(t * TILE, TILE), TILE)
            both = pl.ds(pl.multiple_of(base + 2 * now * half, 256), 2 * half)
            update = dot(b_ref[mine, pl.ds(0, 2 * half)], x_ref[both, columns]).astype(jnp.bfloat16)
            old = x_ref[rows(now, core), columns].astype(jnp.float32)
            x_ref[rows(later, core), columns] = (COEF_A * old + update.astype(jnp.float32)).astype(jnp.bfloat16)
            x_copy(later, columns).start()
            return c

        lax.fori_loop(0, n_long // TILE, apply, 0)
        return carry

    lax.fori_loop(0, NS_STEPS, step, 0)
    x_copy(NS_STEPS % 2, pl.ds(0, n_long)).wait()


def orthogonalize(jobs, stacks, collective_id, keep=False, late=None):
    def whole(shapes, axes, given):
        shorts = [shape[1] * (GROUP if axis == 0 else 1) for shape, axis in zip(shapes, axes)]
        return [(stack, k, chip, turn, axes[stack], shorts[stack]) for stack, k, chip, turn in given]

    shapes, axes = [rows.shape for rows, _ in stacks], [axis for _, axis in stacks]
    full = whole(shapes, axes, jobs)
    n_long = shapes[0][2] * (GROUP if axes[0] == 1 else 1)
    n_pad = padded(max(job[5] for job in full))
    x_rows = sum(rows_of_turn(full, turn) for turn in range(2))
    n_jobs, chips = len(jobs), GROUP // 2
    dma, bf16 = pltpu.SemaphoreType.DMA, jnp.bfloat16
    args = [rows for rows, _ in stacks]
    kept_rows = max((job[3] + 1) * job[5] for job in full)
    out_shape = [jax.ShapeDtypeStruct((kept_rows, n_long), bf16)] if keep else [jax.ShapeDtypeStruct(shape, bf16) for shape in shapes]
    scratch = [pltpu.VMEM((x_rows, n_long), bf16), pltpu.VMEM((n_pad // 2, n_pad), bf16),
               pltpu.VMEM((n_pad // 2, n_pad), bf16), pltpu.VMEM((2, n_pad // 2, n_pad // 2), bf16),
               dma((n_jobs,)), dma((n_jobs, chips)), dma((n_jobs, chips)), dma((n_jobs, chips)), dma((n_jobs, chips)),
               dma((n_jobs,)), dma((n_jobs,)), dma((4,)), dma((4,))]
    full_late = []
    if late is not None:
        late_jobs, late_shapes, late_axes, kept = late
        full_late = whole(late_shapes, late_axes, late_jobs)
        args.append(kept)
        out_shape += [jax.ShapeDtypeStruct(shape, bf16) for shape in late_shapes]
        scratch += [dma((len(late_jobs), chips)), dma((len(late_jobs),)), dma((len(late_jobs), 2))]
        scratch += [pltpu.VMEM((2,) + tuple(shape[1:]), bf16) for shape in late_shapes]
    return pl.pallas_call(
        functools.partial(ortho_kernel, full, full_late, keep),
        out_shape=out_shape,
        in_specs=[pl.BlockSpec(memory_space=pl.ANY)] * len(args),
        out_specs=[pl.BlockSpec(memory_space=pl.ANY)] * len(out_shape),
        scratch_shapes=scratch,
        compiler_params=pltpu.CompilerParams(collective_id=collective_id, has_side_effects=True, vmem_limit_bytes=58 << 20),
        cost_estimate=pl.CostEstimate(flops=2_000_000_000, bytes_accessed=16 << 20, transcendentals=0),
        name=f'ortho{collective_id}',
    )(*args)


SLOTS = 5


def reduce_kernel(n_chunks, per_matrix, grad_ref, out_ref, own_ref, pair_ref, first_ref, second_ref, sum_ref,
                  load_sem, pair_send, pair_recv, first_send, first_recv, second_send, second_recv, out_sem):
    me = lax.axis_index('data')
    y, x, core = me // 4, (me // 2) % 2, me % 2
    greet_all(me)
    chunk = own_ref.shape[3]
    half = chunk // 2
    parts = (pl.ds(0, half), pl.ds(half, half))
    over_core, over_x, over_y = me + 1 - 2 * core, me + 2 - 4 * x, me + 4 - 8 * y

    def remote(src, dst, send, recv, target):
        return pltpu.make_async_remote_copy(src_ref=src, dst_ref=dst, send_sem=send, recv_sem=recv,
                                            device_id={'data': target}, device_id_type=pl.DeviceIdType.MESH)

    def rows_of(c):
        return pl.ds(pl.multiple_of((c % per_matrix) * chunk, chunk), chunk)

    def load(c):
        return pltpu.make_async_copy(grad_ref.at[c // per_matrix, :, :, core, rows_of(c)], own_ref.at[c % SLOTS], load_sem.at[c % SLOTS])

    def pair(c):
        return remote(grad_ref.at[c // per_matrix, :, :, 1 - core, rows_of(c)], pair_ref.at[c % SLOTS],
                      pair_send.at[c % SLOTS], pair_recv.at[c % SLOTS], over_core)

    def first(c):
        slot = c % SLOTS
        return (remote(own_ref.at[slot, :, 1 - x, parts[0]], first_ref.at[slot, 0], first_send.at[slot, 0], first_recv.at[slot, 0], over_x),
                remote(own_ref.at[slot, 1 - y, :, parts[1]], first_ref.at[slot, 1], first_send.at[slot, 1], first_recv.at[slot, 1], over_y))

    def second(c):
        slot = c % SLOTS
        return (remote(own_ref.at[slot, 1 - y, x, parts[0]], second_ref.at[slot, 0], second_send.at[slot, 0], second_recv.at[slot, 0], over_y),
                remote(own_ref.at[slot, y, 1 - x, parts[1]], second_ref.at[slot, 1], second_send.at[slot, 1], second_recv.at[slot, 1], over_x))

    def store(c):
        return pltpu.make_async_copy(sum_ref.at[c % SLOTS], out_ref.at[c // per_matrix, rows_of(c)], out_sem.at[c % SLOTS])

    def during(c, body):
        pl.when(jnp.logical_and(c >= 0, c < n_chunks))(lambda: body(c))

    def finish(c):
        slot = c % SLOTS
        for copy in second(c):
            copy.wait()
        pl.when(c >= SLOTS)(lambda: store(c - SLOTS).wait())
        for side in range(2):
            sum_ref[slot, parts[side]] = own_ref[slot, y, x, parts[side]] + second_ref[slot, side]
        store(c).start()

    def middle(c):
        slot = c % SLOTS
        for copy in first(c):
            copy.wait()
        for other in range(2):
            own_ref[slot, other, x, parts[0]] += first_ref[slot, 0, other]
            own_ref[slot, y, other, parts[1]] += first_ref[slot, 1, other]
        for copy in second(c):
            copy.start()

    def begin(c):
        slot = c % SLOTS
        load(c).wait()
        pair(c).wait()
        own_ref[slot] += pair_ref[slot]
        for copy in first(c):
            copy.start()

    def fetch(c):
        load(c).start()
        pair(c).start()

    def visit(t, carry):
        during(t - 5, finish)
        during(t - 3, middle)
        during(t - 1, begin)
        during(t, fetch)
        return carry

    lax.fori_loop(0, n_chunks + 5, visit, 0)
    for c in range(max(0, n_chunks - SLOTS), n_chunks):
        store(c).wait()


def reduce_rows_kernel(grad, chunk, collective_id):
    count, n_rows, n_cols = grad.shape
    rows = n_rows // GROUP
    per_matrix = rows // chunk
    dma, vmem = pltpu.SemaphoreType.DMA, lambda *shape: pltpu.VMEM(shape, jnp.float32)
    return pl.pallas_call(
        functools.partial(reduce_kernel, count * per_matrix, per_matrix),
        out_shape=jax.ShapeDtypeStruct((count, rows, n_cols), jnp.float32),
        in_specs=[pl.BlockSpec(memory_space=pl.ANY)],
        out_specs=pl.BlockSpec(memory_space=pl.ANY),
        scratch_shapes=[vmem(SLOTS, 2, 2, chunk, n_cols), vmem(SLOTS, 2, 2, chunk, n_cols), vmem(SLOTS, 2, 2, chunk // 2, n_cols),
                        vmem(SLOTS, 2, chunk // 2, n_cols), vmem(SLOTS, chunk, n_cols),
                        dma((SLOTS,)), dma((SLOTS,)), dma((SLOTS,)), dma((SLOTS, 2)), dma((SLOTS, 2)), dma((SLOTS, 2)), dma((SLOTS, 2)),
                        dma((SLOTS,))],
        compiler_params=pltpu.CompilerParams(collective_id=collective_id, has_side_effects=True, vmem_limit_bytes=40 << 20),
        cost_estimate=pl.CostEstimate(flops=1_000_000_000, bytes_accessed=64 << 20, transcendentals=0),
        name=f'reduce{collective_id}',
    )(grad.reshape(count, 2, 2, 2, rows, n_cols))


def momentum(grad_rows, mom_old):
    mom_new = MOMENTUM * mom_old + grad_rows / GROUP
    return mom_new, jnp.sum(mom_new * mom_new, axis=(1, 2))


def to_send(mom_new, norm_sq):
    return (mom_new / (jnp.sqrt(norm_sq)[:, None, None] + EPSILON)).astype(jnp.bfloat16)


def turned_kernel(norm_ref, mom_ref, out_ref):
    out_ref[0] = (mom_ref[0] / norm_ref[pl.program_id(0)]).astype(jnp.bfloat16).T


def to_send_turned(mom_new, norm_sq):
    count, rows, cols = mom_new.shape
    wide = cols
    return pl.pallas_call(
        turned_kernel,
        grid=(count, cols // wide),
        out_shape=jax.ShapeDtypeStruct((count, cols, rows), jnp.bfloat16),
        in_specs=[pl.BlockSpec(memory_space=pltpu.SMEM), pl.BlockSpec((1, rows, wide), lambda k, j: (k, 0, j))],
        out_specs=pl.BlockSpec((1, wide, rows), lambda k, j: (k, j, 0)),
        name='to_send_turned',
    )(jnp.sqrt(norm_sq) + EPSILON, mom_new)


def weights_kernel(scale, ortho_ref, master_ref, new_ref, short_ref):
    ortho = ortho_ref[0].T.astype(jnp.float32)
    new = master_ref[0] - LEARN_RATE * (scale * ortho + WEIGHT_DECAY * master_ref[0])
    new_ref[0] = new
    short_ref[0] = new.astype(jnp.bfloat16)


def new_weights_turned(ortho_turned, master_old, n_rows, n_cols):
    count, rows, cols = master_old.shape
    wide = cols
    straight = pl.BlockSpec((1, rows, wide), lambda k, j: (k, 0, j))
    return pl.pallas_call(
        functools.partial(weights_kernel, 0.2 * math.sqrt(max(n_rows, n_cols))),
        grid=(count, cols // wide),
        out_shape=[jax.ShapeDtypeStruct(master_old.shape, jnp.float32), jax.ShapeDtypeStruct(master_old.shape, jnp.bfloat16)],
        in_specs=[pl.BlockSpec((1, wide, rows), lambda k, j: (k, j, 0)), straight],
        out_specs=[straight, straight],
        name='new_weights_turned',
    )(ortho_turned, master_old)


def new_weights(ortho_rows, master_old, n_rows, n_cols):
    scale = 0.2 * math.sqrt(max(n_rows, n_cols))
    master_new = master_old - LEARN_RATE * (scale * ortho_rows.astype(jnp.float32) + WEIGHT_DECAY * master_old)
    return master_new, master_new.astype(jnp.bfloat16)


def solution(mesh):
    grad_spec = P(('stage', 'data'), None, None, None)
    row_spec = P('stage', 'data', None)

    def step_local(g_attn, m_attn, w_attn, g_up, m_up, w_up, g_down, m_down, w_down):
        def reduce_rows(grad):
            return lax.psum_scatter(grad[0], 'data', scatter_dimension=1, tiled=True)

        r_attn = reduce_rows(g_attn)
        r_down = reduce_rows(g_down)
        r_up = reduce_rows_kernel(g_up[0], 32, 7)
        r_attn, r_up = lax.optimization_barrier((r_attn, r_up))

        mn_attn, part_attn = momentum(r_attn, m_attn)
        mn_up, part_up = momentum(r_up, m_up)
        parts = sum_over_data(jnp.concatenate([part_attn, part_up]), 0)
        x_attn = to_send(mn_attn, parts[:2])
        x_up = to_send_turned(mn_up, parts[2:])
        kept, = orthogonalize(FIRST_JOBS, [(x_attn, 0), (x_up, 1)], 1, keep=True)

        r_down, kept = lax.optimization_barrier((r_down, kept))
        mn_down, part_down = momentum(r_down, m_down)
        x_down = to_send(mn_down, sum_over_data(part_down, 4))
        or_down, or_attn, or_up = orthogonalize(LAST_JOBS, [(x_down, 0)], 5, late=(FIRST_JOBS, (x_attn.shape, x_up.shape), (0, 1), kept))
        wn_attn, wb_attn = new_weights(or_attn, w_attn, 2048, 2048)
        wn_up, wb_up = new_weights_turned(or_up, w_up, 2048, 1408)
        wn_down, wb_down = new_weights(or_down, w_down, 1408, 2048)
        return (mn_attn, wn_attn, wb_attn, mn_up, wn_up, wb_up, mn_down, wn_down, wb_down)

    in_specs = (grad_spec, row_spec, row_spec) * 3
    out_specs = (row_spec,) * 9
    return jax.shard_map(step_local, mesh=mesh, in_specs=in_specs, out_specs=out_specs, check_vma=False)
```

```python
import math
import functools
import jax
import jax.numpy as jnp
from jax import lax
from jax.experimental import pallas as pl
from jax.experimental.pallas import tpu as pltpu
from jax.sharding import PartitionSpec as P

MOMENTUM = 0.95
LEARN_RATE = 0.25
WEIGHT_DECAY = 0.2
EPSILON = 1e-7
COEF_A = 3.4445
COEF_B = -4.7750
COEF_C = 2.0315
NS_STEPS = 5
GROUP = 8
FIRST_JOBS = ((0, 0, 0, 0), (0, 1, 3, 0), (1, 0, 1, 0), (1, 2, 2, 0), (1, 1, 1, 1), (1, 3, 2, 1))
LAST_JOBS = ((0, 0, 0, 0), (0, 1, 1, 0), (0, 2, 2, 0), (0, 3, 3, 0))


def greet_all(me):
    barrier = pltpu.get_barrier_semaphore()
    for step in range(1, GROUP):
        pl.semaphore_signal(barrier, inc=1, device_id={'data': lax.rem(me + step, GROUP)}, device_id_type=pl.DeviceIdType.MESH)
    pl.semaphore_wait(barrier, GROUP - 1)


def share_kernel(part_ref, all_ref, send_sem, recv_sem):
    me = lax.axis_index('data')
    greet_all(me)
    copies = []
    for step in range(1, GROUP):
        copies.append(pltpu.make_async_remote_copy(
            src_ref=part_ref, dst_ref=all_ref.at[step], send_sem=send_sem.at[step], recv_sem=recv_sem.at[step],
            device_id={'data': lax.rem(me + step, GROUP)}, device_id_type=pl.DeviceIdType.MESH))
    for copy in copies:
        copy.start()
    all_ref[0] = part_ref[...]
    for copy in copies:
        copy.wait()


def sum_over_data(partial, collective_id):
    count = partial.shape[0]
    tile = jnp.broadcast_to(jnp.pad(partial, (0, 8 - count))[:, None], (8, 128))
    shared = pl.pallas_call(
        share_kernel,
        out_shape=jax.ShapeDtypeStruct((GROUP, 8, 128), jnp.float32),
        in_specs=[pl.BlockSpec(memory_space=pltpu.VMEM)],
        out_specs=pl.BlockSpec(memory_space=pltpu.VMEM),
        scratch_shapes=[pltpu.SemaphoreType.DMA((GROUP,)), pltpu.SemaphoreType.DMA((GROUP,))],
        compiler_params=pltpu.CompilerParams(collective_id=collective_id, has_side_effects=True),
        cost_estimate=pl.CostEstimate(flops=20_000_000, bytes_accessed=65536, transcendentals=0),
        name=f'share{collective_id}',
    )(tile)
    me = lax.axis_index('data')
    ordered = jnp.take(shared[:, :, 0], lax.rem(me - jnp.arange(GROUP) + GROUP, GROUP), axis=0)
    return jnp.sum(ordered, axis=0)[:count]


def block_of(ref, device, size, axis):
    start = pl.multiple_of(device * size, size)
    return ref.at[pl.ds(start, size), :] if axis == 0 else ref.at[:, pl.ds(start, size)]


def normalize(me, mom_ref, part_ref, all_ref, wide_ref, x_ref, send_sem, recv_sem, load_sem):
    def share(source, target):
        return pltpu.make_async_remote_copy(
            src_ref=part_ref, dst_ref=all_ref.at[source], send_sem=send_sem.at[target], recv_sem=recv_sem.at[source],
            device_id={'data': target}, device_id_type=pl.DeviceIdType.MESH)

    others = [lax.rem(me + step, GROUP) for step in range(1, GROUP)]
    for other in others:
        share(me, other).start()
    load = pltpu.make_async_copy(mom_ref, wide_ref, load_sem)
    load.start()
    all_ref[me] = part_ref[...]
    for other in others:
        share(me, other).wait_send()
        share(other, other).wait_recv()
    total = all_ref[0]
    for device in range(1, GROUP):
        total += all_ref[device]
    norm = jnp.sqrt(total) + EPSILON
    load.wait()
    for k in range(mom_ref.shape[0]):
        x_ref[k] = (wide_ref[k] / norm[k:k + 1, :1]).astype(jnp.bfloat16)
    return x_ref


def ortho_kernel(jobs, late, keep, raw, *refs):
    n_stacks = 1 + max(job[0] for job in jobs)
    n_late = 1 + max([job[0] for job in late], default=-1)
    n_in = n_stacks + raw + (n_late > 0)
    n_out = 1 if keep else n_stacks
    ins, kept_in = refs[:n_stacks], refs[n_in - 1]
    outs, late_outs = refs[n_in:n_in + n_out], refs[n_in + n_out:n_in + n_out + n_late]
    scratch = refs[n_in + n_out + n_late:]
    (x_ref, a_ref, b_ref, far_ref, send_sem, recv_sem, pass_sem, passed_sem, back_sem, got_sem, own_sem,
     tile_send, tile_recv) = scratch[:13]
    me = lax.axis_index('data')
    chip, core = me // 2, me % 2
    partner = me + 1 - 2 * core
    greet_all(me)
    if raw:
        ins = (normalize(me, ins[0], refs[n_stacks], *scratch[-6:]),)
    n_long = x_ref.shape[1]
    chips = GROUP // 2
    turn_rows = rows_of_turn(jobs, 0)
    last = NS_STEPS % 2

    def remote(src, dst, send, recv, target):
        return pltpu.make_async_remote_copy(src_ref=src, dst_ref=dst, send_sem=send, recv_sem=recv,
                                            device_id={'data': target}, device_id_type=pl.DeviceIdType.MESH)

    def block(job, slot, device):
        _, _, _, turn, axis, n_short = jobs[job]
        size = (n_short if axis == 0 else n_long) // GROUP
        return block_of(x_ref.at[pl.ds(turn * turn_rows + slot * padded(n_short), n_short)], device, size, axis)

    def rows_in(job):
        return ins[jobs[job][0]].at[jobs[job][1]]

    def rows_out(job):
        return outs[jobs[job][0]].at[jobs[job][1]]

    def collect(job, source):
        return remote(rows_in(job), block(job, 0, 2 * source + core), send_sem.at[job], recv_sem.at[job, source], 2 * jobs[job][2] + core)

    def collect_own(job):
        return pltpu.make_async_copy(rows_in(job), block(job, 0, me), own_sem.at[job])

    def pass_on(job, source, side):
        there = block(job, 0, 2 * source + side)
        return remote(there, there, pass_sem.at[job, source], passed_sem.at[job, source], partner)

    def hand_out(job, target):
        return remote(block(job, last, 2 * target + core), rows_out(job), back_sem.at[job, target], got_sem.at[job], 2 * target + core)

    def hand_out_own(job):
        return pltpu.make_async_copy(block(job, last, me), rows_out(job), own_sem.at[job])

    def store(job):
        _, _, _, turn, _, n_short = jobs[job]
        there = x_ref.at[pl.ds(turn * turn_rows + last * padded(n_short), n_short)]
        return pltpu.make_async_copy(there, outs[0].at[pl.ds(turn * n_short, n_short)], own_sem.at[job])

    def late_block(index, device):
        _, _, _, turn, axis, n_short = late[index]
        size = (n_short if axis == 0 else n_long) // GROUP
        return block_of(kept_in.at[pl.ds(turn * n_short, n_short)], device, size, axis)

    def late_out(index):
        return late_outs[late[index][0]].at[late[index][1]]

    def late_hand_out(index, target):
        return remote(late_block(index, 2 * target + core), late_out(index), scratch[13].at[index, target], scratch[14].at[index], 2 * target + core)

    def late_own(index, outward):
        room = scratch[16 + late[index][0]].at[late[index][3]]
        if outward:
            return pltpu.make_async_copy(room, late_out(index), scratch[15].at[index, 1])
        return pltpu.make_async_copy(late_block(index, me), room, scratch[15].at[index, 0])

    def each_late(owning, other=None):
        for index, job in enumerate(late):
            pl.when(chip == job[2])(functools.partial(owning, index))
            if other is not None:
                pl.when(chip != job[2])(functools.partial(other, index))

    def late_begin(index):
        late_own(index, False).start()
        for target in range(chips):
            if target != late[index][2]:
                late_hand_out(index, target).start()

    def late_middle(index):
        late_own(index, False).wait()
        late_own(index, True).start()

    def late_end(index):
        late_own(index, True).wait()
        for target in range(chips):
            if target != late[index][2]:
                late_hand_out(index, target).wait_send()

    for job, (_, _, owner, turn, _, n_short) in enumerate(jobs):
        @pl.when(chip != owner)
        def _():
            collect(job, chip).start()

        @pl.when(chip == owner)
        def _():
            collect_own(job).start()
            n_pad = padded(n_short)
            if n_pad > n_short:
                for slot in range(2):
                    start = turn * turn_rows + slot * n_pad
                    x_ref[start + n_short:start + n_pad, :] = jnp.zeros((n_pad - n_short, n_long), jnp.bfloat16)

    def receive(job):
        collect_own(job).wait()
        pass_on(job, jobs[job][2], core).start()
        for source in range(chips):
            if source != jobs[job][2]:
                collect(job, source).wait_recv()
                pass_on(job, source, core).start()
        for source in range(chips):
            pass_on(job, source, core).wait_send()
            pass_on(job, source, 1 - core).wait_recv()

    def give_back(t, job):
        columns = pl.ds(pl.multiple_of(t * TILE, TILE), TILE)
        for target in range(chips):
            here, there = block(job, last, 2 * target + core).at[:, columns], rows_out(job).at[:, columns]
            if target == jobs[job][2]:
                pltpu.make_async_copy(here, there, own_sem.at[job]).start()
            else:
                remote(here, there, back_sem.at[job, target], got_sem.at[job], 2 * target + core).start()

    for n_short in sorted({job[5] for job in jobs}):
        mine = [job for job in range(len(jobs)) if jobs[job][5] == n_short]

        def work(turn, carry):
            def each(body):
                for job in mine:
                    pl.when(jnp.logical_and(chip == jobs[job][2], turn == jobs[job][3]))(functools.partial(body, job))

            each(receive)
            each_late(late_begin)
            newton_schulz(padded(n_short) // 2, core, partner, remote, x_ref, turn * turn_rows, a_ref, b_ref, far_ref, tile_send, tile_recv,
                          None if keep else lambda t: each(functools.partial(give_back, t)))
            if keep:
                each(lambda job: store(job).start())
            each_late(late_middle)
            return carry

        @pl.when(functools.reduce(jnp.logical_or, [chip == jobs[job][2] for job in mine]))
        def _():
            lax.fori_loop(0, 1 + max(jobs[job][3] for job in mine), work, 0)

    for job, (_, _, owner, _, _, _) in enumerate(jobs):
        @pl.when(chip == owner)
        def _():
            if keep:
                store(job).wait()
                return
            hand_out_own(job).wait()
            for target in range(chips):
                if target != owner:
                    hand_out(job, target).wait_send()

        @pl.when(chip != owner)
        def _():
            collect(job, chip).wait_send()
            if not keep:
                hand_out(job, chip).wait_recv()
    each_late(late_end, lambda index: late_hand_out(index, chip).wait_recv())


def padded(n_short):
    return -(-n_short // TILE) * TILE


def rows_of_turn(jobs, turn):
    return 2 * padded(max([job[5] for job in jobs if job[3] == turn], default=0))


TILE = 512


def newton_schulz(half, core, partner, remote, x_ref, base, a_ref, b_ref, far_ref, tile_send, tile_recv, finish=None):
    n_long = x_ref.shape[1]
    near, far = (pl.ds(pl.multiple_of(side * half, half), half) for side in (core, 1 - core))
    mine = pl.ds(0, half)

    def rows(slot, side):
        return pl.ds(pl.multiple_of(base + (2 * slot + side) * half, 256), half)

    def a_copy(parity):
        return remote(a_ref.at[mine, near], far_ref.at[parity, mine, mine], tile_send.at[parity], tile_recv.at[parity], partner)

    def x_copy(slot, columns):
        there = x_ref.at[rows(slot, core), columns]
        return remote(there, there, tile_send.at[2 + slot], tile_recv.at[2 + slot], partner)

    def end_copy(t):
        there = x_ref.at[rows(NS_STEPS % 2, core), pl.ds(pl.multiple_of(t * TILE, TILE), TILE)]
        return remote(there, there, tile_send.at[4 + t], tile_recv.at[4 + t], partner)

    def end(t):
        end_copy(t).wait()
        finish(t)

    def dot(left, right):
        return jnp.dot(left, right, preferred_element_type=jnp.float32)

    def dot_t(left, right):
        return lax.dot_general(left, right, (((1,), (1,)), ((), ())), preferred_element_type=jnp.float32)

    def piece(index):
        return pl.ds(pl.multiple_of(index * (half // 2), half // 2), half // 2)

    def poly(columns, square):
        def visit(index, c):
            band = piece(index)
            tile = COEF_B * a_ref[band, columns].astype(jnp.float32)
            tile += COEF_C * square(band).astype(jnp.bfloat16).astype(jnp.float32)
            b_ref[band, columns] = tile.astype(jnp.bfloat16)
            return c
        lax.fori_loop(0, 2, visit, 0)

    def step(count, carry):
        now, later = count % 2, (count + 1) % 2

        def gram(turn, c):
            side = core + (turn // 2) * (1 - 2 * core)
            band, columns = piece(turn % 2), pl.ds(pl.multiple_of(side * half, half), half)
            left = x_ref[pl.ds(pl.multiple_of(base + (2 * now + core) * half + (turn % 2) * (half // 2), 128), half // 2), :]
            a_ref[band, columns] = dot_t(left, x_ref[rows(now, side), :]).astype(jnp.bfloat16)
            pl.when(turn == 1)(lambda: a_copy(now).start())
            pl.when(jnp.logical_and(turn == 1, count > 0))(lambda: x_copy(now, pl.ds(0, n_long)).wait())
            return c

        lax.fori_loop(0, 4, gram, 0)
        poly(near, lambda band: dot(a_ref[band, near], a_ref[mine, near]) + dot_t(a_ref[band, far], a_ref[mine, far]))
        a_copy(now).wait()
        poly(far, lambda band: dot(a_ref[band, near], a_ref[mine, far]) + dot(a_ref[band, far], far_ref[now, mine, mine]))

        def apply(t, c):
            columns = pl.ds(pl.multiple_of(t * TILE, TILE), TILE)
            both = pl.ds(pl.multiple_of(base + 2 * now * half, 256), 2 * half)
            update = dot(b_ref[mine, pl.ds(0, 2 * half)], x_ref[both, columns]).astype(jnp.bfloat16)
            old = x_ref[rows(now, core), columns].astype(jnp.float32)
            x_ref[rows(later, core), columns] = (COEF_A * old + update.astype(jnp.float32)).astype(jnp.bfloat16)
            if finish is None:
                x_copy(later, columns).start()
                return c
            is_last = count == NS_STEPS - 1
            pl.when(jnp.logical_not(is_last))(lambda: x_copy(later, columns).start())
            pl.when(is_last)(lambda: end_copy(t).start())
            pl.when(jnp.logical_and(is_last, t > 0))(lambda: end(t - 1))
            return c

        lax.fori_loop(0, n_long // TILE, apply, 0)
        return carry

    lax.fori_loop(0, NS_STEPS, step, 0)
    if finish is None:
        x_copy(NS_STEPS % 2, pl.ds(0, n_long)).wait()
    else:
        end(n_long // TILE - 1)


def orthogonalize(jobs, stacks, collective_id, keep=False, late=None, part=None):
    def whole(shapes, axes, given):
        shorts = [shape[1] * (GROUP if axis == 0 else 1) for shape, axis in zip(shapes, axes)]
        return [(stack, k, chip, turn, axes[stack], shorts[stack]) for stack, k, chip, turn in given]

    shapes, axes = [rows.shape for rows, _ in stacks], [axis for _, axis in stacks]
    full = whole(shapes, axes, jobs)
    n_long = shapes[0][2] * (GROUP if axes[0] == 1 else 1)
    n_pad = padded(max(job[5] for job in full))
    x_rows = sum(rows_of_turn(full, turn) for turn in range(2))
    n_jobs, chips = len(jobs), GROUP // 2
    dma, bf16 = pltpu.SemaphoreType.DMA, jnp.bfloat16
    args = [rows for rows, _ in stacks]
    if part is not None:
        args.append(jnp.broadcast_to(jnp.pad(part, (0, 8 - part.shape[0]))[:, None], (8, 128)))
    kept_rows = max((job[3] + 1) * job[5] for job in full)
    out_shape = [jax.ShapeDtypeStruct((kept_rows, n_long), bf16)] if keep else [jax.ShapeDtypeStruct(shape, bf16) for shape in shapes]
    scratch = [pltpu.VMEM((x_rows, n_long), bf16), pltpu.VMEM((n_pad // 2, n_pad), bf16),
               pltpu.VMEM((n_pad // 2, n_pad), bf16), pltpu.VMEM((2, n_pad // 2, n_pad // 2), bf16),
               dma((n_jobs,)), dma((n_jobs, chips)), dma((n_jobs, chips)), dma((n_jobs, chips)), dma((n_jobs, chips)),
               dma((n_jobs,)), dma((n_jobs,)), dma((4 + n_long // TILE,)), dma((4 + n_long // TILE,))]
    full_late = []
    if late is not None:
        late_jobs, late_shapes, late_axes, kept = late
        full_late = whole(late_shapes, late_axes, late_jobs)
        args.append(kept)
        out_shape += [jax.ShapeDtypeStruct(shape, bf16) for shape in late_shapes]
        scratch += [dma((len(late_jobs), chips)), dma((len(late_jobs),)), dma((len(late_jobs), 2))]
        scratch += [pltpu.VMEM((2,) + tuple(shape[1:]), bf16) for shape in late_shapes]
    specs = [pl.BlockSpec(memory_space=pl.ANY)] * len(args)
    if part is not None:
        specs[len(stacks)] = pl.BlockSpec(memory_space=pltpu.VMEM)
        scratch += [pltpu.VMEM((GROUP, 8, 128), jnp.float32), pltpu.VMEM(shapes[0], jnp.float32), pltpu.VMEM(shapes[0], bf16),
                    dma((GROUP,)), dma((GROUP,)), dma]
    return pl.pallas_call(
        functools.partial(ortho_kernel, full, full_late, keep, part is not None),
        out_shape=out_shape,
        in_specs=specs,
        out_specs=[pl.BlockSpec(memory_space=pl.ANY)] * len(out_shape),
        scratch_shapes=scratch,
        compiler_params=pltpu.CompilerParams(collective_id=collective_id, has_side_effects=True, vmem_limit_bytes=58 << 20),
        cost_estimate=pl.CostEstimate(flops=2_000_000_000, bytes_accessed=16 << 20, transcendentals=0),
        name=f'ortho{collective_id}',
    )(*args)


SLOTS = 5


def reduce_kernel(n_chunks, per_matrix, grad_ref, out_ref, own_ref, pair_ref, first_ref, second_ref, sum_ref,
                  load_sem, pair_send, pair_recv, first_send, first_recv, second_send, second_recv, out_sem):
    me = lax.axis_index('data')
    y, x, core = me // 4, (me // 2) % 2, me % 2
    greet_all(me)
    chunk = own_ref.shape[3]
    half = chunk // 2
    parts = (pl.ds(0, half), pl.ds(half, half))
    over_core, over_x, over_y = me + 1 - 2 * core, me + 2 - 4 * x, me + 4 - 8 * y

    def remote(src, dst, send, recv, target):
        return pltpu.make_async_remote_copy(src_ref=src, dst_ref=dst, send_sem=send, recv_sem=recv,
                                            device_id={'data': target}, device_id_type=pl.DeviceIdType.MESH)

    def rows_of(c):
        return pl.ds(pl.multiple_of((c % per_matrix) * chunk, chunk), chunk)

    def load(c):
        return pltpu.make_async_copy(grad_ref.at[c // per_matrix, :, :, core, rows_of(c)], own_ref.at[c % SLOTS], load_sem.at[c % SLOTS])

    def pair(c):
        return remote(grad_ref.at[c // per_matrix, :, :, 1 - core, rows_of(c)], pair_ref.at[c % SLOTS],
                      pair_send.at[c % SLOTS], pair_recv.at[c % SLOTS], over_core)

    def first(c):
        slot = c % SLOTS
        return (remote(own_ref.at[slot, :, 1 - x, parts[0]], first_ref.at[slot, 0], first_send.at[slot, 0], first_recv.at[slot, 0], over_x),
                remote(own_ref.at[slot, 1 - y, :, parts[1]], first_ref.at[slot, 1], first_send.at[slot, 1], first_recv.at[slot, 1], over_y))

    def second(c):
        slot = c % SLOTS
        return (remote(own_ref.at[slot, 1 - y, x, parts[0]], second_ref.at[slot, 0], second_send.at[slot, 0], second_recv.at[slot, 0], over_y),
                remote(own_ref.at[slot, y, 1 - x, parts[1]], second_ref.at[slot, 1], second_send.at[slot, 1], second_recv.at[slot, 1], over_x))

    def store(c):
        return pltpu.make_async_copy(sum_ref.at[c % SLOTS], out_ref.at[c // per_matrix, rows_of(c)], out_sem.at[c % SLOTS])

    def during(c, body):
        pl.when(jnp.logical_and(c >= 0, c < n_chunks))(lambda: body(c))

    def finish(c):
        slot = c % SLOTS
        for copy in second(c):
            copy.wait()
        pl.when(c >= SLOTS)(lambda: store(c - SLOTS).wait())
        for side in range(2):
            sum_ref[slot, parts[side]] = own_ref[slot, y, x, parts[side]] + second_ref[slot, side]
        store(c).start()

    def middle(c):
        slot = c % SLOTS
        for copy in first(c):
            copy.wait()
        for other in range(2):
            own_ref[slot, other, x, parts[0]] += first_ref[slot, 0, other]
            own_ref[slot, y, other, parts[1]] += first_ref[slot, 1, other]
        for copy in second(c):
            copy.start()

    def begin(c):
        slot = c % SLOTS
        load(c).wait()
        pair(c).wait()
        own_ref[slot] += pair_ref[slot]
        for copy in first(c):
            copy.start()

    def fetch(c):
        load(c).start()
        pair(c).start()

    def visit(t, carry):
        during(t - 5, finish)
        during(t - 3, middle)
        during(t - 1, begin)
        during(t, fetch)
        return carry

    lax.fori_loop(0, n_chunks + 5, visit, 0)
    for c in range(max(0, n_chunks - SLOTS), n_chunks):
        store(c).wait()


def reduce_rows_kernel(grad, chunk, collective_id):
    count, n_rows, n_cols = grad.shape
    rows = n_rows // GROUP
    per_matrix = rows // chunk
    dma, vmem = pltpu.SemaphoreType.DMA, lambda *shape: pltpu.VMEM(shape, jnp.float32)
    return pl.pallas_call(
        functools.partial(reduce_kernel, count * per_matrix, per_matrix),
        out_shape=jax.ShapeDtypeStruct((count, rows, n_cols), jnp.float32),
        in_specs=[pl.BlockSpec(memory_space=pl.ANY)],
        out_specs=pl.BlockSpec(memory_space=pl.ANY),
        scratch_shapes=[vmem(SLOTS, 2, 2, chunk, n_cols), vmem(SLOTS, 2, 2, chunk, n_cols), vmem(SLOTS, 2, 2, chunk // 2, n_cols),
                        vmem(SLOTS, 2, chunk // 2, n_cols), vmem(SLOTS, chunk, n_cols),
                        dma((SLOTS,)), dma((SLOTS,)), dma((SLOTS,)), dma((SLOTS, 2)), dma((SLOTS, 2)), dma((SLOTS, 2)), dma((SLOTS, 2)),
                        dma((SLOTS,))],
        compiler_params=pltpu.CompilerParams(collective_id=collective_id, has_side_effects=True, vmem_limit_bytes=40 << 20),
        cost_estimate=pl.CostEstimate(flops=1_000_000_000, bytes_accessed=64 << 20, transcendentals=0),
        name=f'reduce{collective_id}',
    )(grad.reshape(count, 2, 2, 2, rows, n_cols))


def momentum(grad_rows, mom_old):
    mom_new = MOMENTUM * mom_old + grad_rows / GROUP
    return mom_new, jnp.sum(mom_new * mom_new, axis=(1, 2))


def to_send(mom_new, norm_sq):
    return (mom_new / (jnp.sqrt(norm_sq)[:, None, None] + EPSILON)).astype(jnp.bfloat16)


def turned_kernel(norm_ref, mom_ref, out_ref):
    out_ref[0] = (mom_ref[0] / norm_ref[pl.program_id(0)]).astype(jnp.bfloat16).T


def to_send_turned(mom_new, norm_sq):
    count, rows, cols = mom_new.shape
    wide = cols
    return pl.pallas_call(
        turned_kernel,
        grid=(count, cols // wide),
        out_shape=jax.ShapeDtypeStruct((count, cols, rows), jnp.bfloat16),
        in_specs=[pl.BlockSpec(memory_space=pltpu.SMEM), pl.BlockSpec((1, rows, wide), lambda k, j: (k, 0, j))],
        out_specs=pl.BlockSpec((1, wide, rows), lambda k, j: (k, j, 0)),
        name='to_send_turned',
    )(jnp.sqrt(norm_sq) + EPSILON, mom_new)


def weights_kernel(scale, ortho_ref, master_ref, new_ref, short_ref):
    ortho = ortho_ref[0].T.astype(jnp.float32)
    new = master_ref[0] - LEARN_RATE * (scale * ortho + WEIGHT_DECAY * master_ref[0])
    new_ref[0] = new
    short_ref[0] = new.astype(jnp.bfloat16)


def new_weights_turned(ortho_turned, master_old, n_rows, n_cols):
    count, rows, cols = master_old.shape
    wide = cols
    straight = pl.BlockSpec((1, rows, wide), lambda k, j: (k, 0, j))
    return pl.pallas_call(
        functools.partial(weights_kernel, 0.2 * math.sqrt(max(n_rows, n_cols))),
        grid=(count, cols // wide),
        out_shape=[jax.ShapeDtypeStruct(master_old.shape, jnp.float32), jax.ShapeDtypeStruct(master_old.shape, jnp.bfloat16)],
        in_specs=[pl.BlockSpec((1, wide, rows), lambda k, j: (k, j, 0)), straight],
        out_specs=[straight, straight],
        name='new_weights_turned',
    )(ortho_turned, master_old)


def new_weights(ortho_rows, master_old, n_rows, n_cols):
    scale = 0.2 * math.sqrt(max(n_rows, n_cols))
    master_new = master_old - LEARN_RATE * (scale * ortho_rows.astype(jnp.float32) + WEIGHT_DECAY * master_old)
    return master_new, master_new.astype(jnp.bfloat16)


def solution(mesh):
    grad_spec = P(('stage', 'data'), None, None, None)
    row_spec = P('stage', 'data', None)

    def step_local(g_attn, m_attn, w_attn, g_up, m_up, w_up, g_down, m_down, w_down):
        def reduce_rows(grad):
            return lax.psum_scatter(grad[0], 'data', scatter_dimension=1, tiled=True)

        r_attn = reduce_rows(g_attn)
        r_down = reduce_rows(g_down)
        r_up = reduce_rows_kernel(g_up[0], 32, 7)
        r_attn, r_up = lax.optimization_barrier((r_attn, r_up))

        mn_attn, part_attn = momentum(r_attn, m_attn)
        mn_up, part_up = momentum(r_up, m_up)
        parts = sum_over_data(jnp.concatenate([part_attn, part_up]), 0)
        x_attn = to_send(mn_attn, parts[:2])
        x_up = to_send_turned(mn_up, parts[2:])
        kept, = orthogonalize(FIRST_JOBS, [(x_attn, 0), (x_up, 1)], 1, keep=True)

        r_down, kept = lax.optimization_barrier((r_down, kept))
        mn_down, part_down = momentum(r_down, m_down)
        or_down, or_attn, or_up = orthogonalize(
            LAST_JOBS, [(mn_down, 0)], 5, late=(FIRST_JOBS, (x_attn.shape, x_up.shape), (0, 1), kept), part=part_down)
        wn_attn, wb_attn = new_weights(or_attn, w_attn, 2048, 2048)
        wn_up, wb_up = new_weights_turned(or_up, w_up, 2048, 1408)
        wn_down, wb_down = new_weights(or_down, w_down, 1408, 2048)
        return (mn_attn, wn_attn, wb_attn, mn_up, wn_up, wb_up, mn_down, wn_down, wb_down)

    in_specs = (grad_spec, row_spec, row_spec) * 3
    out_specs = (row_spec,) * 9
    return jax.shard_map(step_local, mesh=mesh, in_specs=in_specs, out_specs=out_specs, check_vma=False)
```
